32 devices in a mesh: det: 8 (over y, x, core), bm: 4 (over z).
Axes of the slice: x: 2, y: 2, z: 4, core: 2. Of those that a mesh axis runs over, the one named last changes fastest.
Arguments:
- sky_alm: bfloat16 [2, 3, 16, 128], P(None, None, 'det'), may hold values from -6 to 6
- beam_blm: bfloat16 [2, 3, 16, 128], P(None, None, 'bm'), may hold values from -2.5 to 2.5
- wigner: bfloat16 [32, 16, 16, 128], P('det', None, 'bm'), may hold values from -0.03125 to 0.03125
- theta_index: int32 [128, 256], P('det'), may hold values from 0 to 3
- phi_index: int32 [128, 256], P('det'), may hold values from 0 to 16383
- psi_index: int32 [128, 256], P('det'), may hold values from 0 to 31
Outputs:
- tod: float32 [128, 256], P('det', 'bm')
The draws below stay inside these ranges and needn't reach their ends.
All inputs are finite; a program needn't handle non-finite values.
Results may differ from the reference program's by a relative error of at most 0.0029.
Values may be sent and summed in bfloat16 or wider, within the bound.
No kernel may reach another device: no remote copies, remote signals or barrier semaphores. Data moves between devices by JAX's collectives and lax.ppermute only.
A program may use at most 64 MiB of HBM per device.

```python
import math
import jax
import jax.numpy as jnp
from jax import lax

LBAND = 128
BEAM_M = 16
NR = 4
SAMP = 256
NPHI = 16384
NPSI = 32
MWIN = 16
CYCLES = 32
DETS = 128
N_DET = 8


def set_ends(drawn, own_key, least, top_value):
    spot = [jax.random.randint(jax.random.fold_in(own_key, axis), (), 0, length) for axis, length in enumerate(drawn.shape)]
    main_axis = drawn.shape.index(max(drawn.shape))
    beside = spot[:main_axis] + [(spot[main_axis] + 1) % drawn.shape[main_axis]] + spot[main_axis + 1:]
    return drawn.at[tuple(spot)].set(least).at[tuple(beside)].set(top_value)


def shard_levels(stream_key, shape, cuts, least, high):
    level, own = 1.0, jax.random.fold_in(stream_key, 6)
    for axis_at, parts in cuts:
        draws = jnp.exp(jax.random.uniform(jax.random.fold_in(own, axis_at), (parts,), jnp.float32, least / len(cuts), high / len(cuts)))
        level = level * jnp.repeat(draws, shape[axis_at] // parts).reshape([-1 if axis == axis_at else 1 for axis in range(len(shape))])
    return level


def bell_draw(rng, extent, deviation, bound, split=(), kind=jnp.bfloat16):
    drawn = deviation * jax.random.normal(rng, extent, jnp.float32)
    if split:
        drawn = drawn * shard_levels(rng, extent, split, -0.22, 0.18)
    return jnp.clip(drawn, -bound, bound).astype(kind)


def setup_inputs(seed: int = 0) -> dict:
    splits = jax.random.split(jax.random.key(seed), 7)
    sky_alm = bell_draw(splits[0], (2, 3, MWIN, LBAND), 1.0, 6.0, ((2, 8),))
    beam_blm = bell_draw(splits[1], (2, 3, BEAM_M, LBAND), 6 ** -0.5, 2.5, ((2, 4),))
    wigner = bell_draw(splits[2], (CYCLES, MWIN, BEAM_M, LBAND), (LBAND * MWIN * BEAM_M) ** -0.5, 0.03125, ((0, 8), (2, 4)))
    theta_index = set_ends(jax.random.randint(splits[3], (DETS, SAMP), 0, NR), jax.random.fold_in(splits[3], 1), 0, NR - 1).astype(jnp.int32)
    phi_index = set_ends(jax.random.randint(splits[4], (DETS, SAMP), 0, NPHI), jax.random.fold_in(splits[4], 1), 0, NPHI - 1).astype(jnp.int32)
    psi_index = set_ends(jax.random.randint(splits[5], (DETS, SAMP), 0, NPSI), jax.random.fold_in(splits[5], 1), 0, NPSI - 1).astype(jnp.int32)
    return dict(sky_alm=sky_alm, beam_blm=beam_blm, wigner=wigner, theta_index=theta_index, phi_index=phi_index, psi_index=psi_index)


TWO_PI = 2.0 * math.pi


def spectra_of(sky, beam):
    sky_full = sky.astype(jnp.float32)[:, :, :, None, :]
    beam_full = beam.astype(jnp.float32)[:, :, None, :, :]
    real_part = jnp.sum(sky_full[0] * beam_full[0] - sky_full[1] * beam_full[1], axis=0)
    imag_part = jnp.sum(sky_full[0] * beam_full[1] + sky_full[1] * beam_full[0], axis=0)
    return jnp.stack([real_part, imag_part]).astype(jnp.bfloat16)


def product_first(left, right):
    dims = (((0,), (0,)), ((), ()))
    return lax.dot_general(left, right, dims, precision=lax.Precision.HIGHEST, preferred_element_type=jnp.float32)


def sample_tod(cube, theta, phi, psi, first_plane):
    cycles = cube.shape[1]
    planes = cube.shape[2]
    modes = cube.shape[3]
    plane_ids = first_plane + jnp.arange(planes, dtype=jnp.int32)
    psi_angle = TWO_PI * ((plane_ids[:, None] * psi[None, :]) % NPSI).astype(jnp.float32) / NPSI
    select = (theta[None, :] == jnp.arange(cycles, dtype=jnp.int32)[:, None]).astype(jnp.float32)
    cos_feat = (select[:, None, :] * jnp.cos(psi_angle)[None]).reshape(cycles * planes, -1)
    sin_feat = (select[:, None, :] * jnp.sin(psi_angle)[None]).reshape(cycles * planes, -1)
    flat = cube.reshape(2, cycles * planes, modes)
    k_real = product_first(flat[0], cos_feat) - product_first(flat[1], sin_feat)
    k_imag = product_first(flat[1], cos_feat) + product_first(flat[0], sin_feat)
    mode_ids = jnp.arange(modes, dtype=jnp.int32)
    phi_angle = TWO_PI * ((mode_ids[:, None] * phi[None, :]) % NPHI).astype(jnp.float32) / NPHI
    return jnp.sum(k_real * jnp.cos(phi_angle) - k_imag * jnp.sin(phi_angle), axis=0)


def reference(sky_alm, beam_blm, wigner, theta_index, phi_index, psi_index):
    spectra = lax.optimization_barrier(spectra_of(sky_alm, beam_blm)).astype(jnp.float32)
    tables = wigner.reshape(N_DET, NR, MWIN, BEAM_M, LBAND)

    def one_group(inputs):
        table, theta, phi, psi = inputs
        cube = jnp.einsum("rmpl,kmpl->krpm", table.astype(jnp.float32), spectra, precision=lax.Precision.HIGHEST)
        return sample_tod(cube, theta, phi, psi, 0)

    tod = lax.map(one_group, (tables, theta_index.reshape(N_DET, -1), phi_index.reshape(N_DET, -1), psi_index.reshape(N_DET, -1)))
    return tod.reshape(DETS, SAMP)
```

```python
import functools
import math

import jax
import jax.numpy as jnp
from jax import lax
from jax.experimental import pallas as pl
from jax.experimental.pallas import tpu as pltpu
from jax.sharding import PartitionSpec as P

NPHI = 16384
NPSI = 32
LANES = 128
SUBLANES = 8

SIN_TERMS = (1.0, -1 / 6, 1 / 120, -1 / 5040, 1 / 362880)
COS_TERMS = (1.0, -1 / 2, 1 / 24, -1 / 720, 1 / 40320)


def kernel_call(body, outs, *args, scalars=1, flops=0):
    spaces = [pltpu.SMEM] * scalars + [pltpu.VMEM] * (len(args) - scalars)
    return pl.pallas_call(
        body,
        out_shape=outs,
        in_specs=[pl.BlockSpec(memory_space=space) for space in spaces],
        out_specs=jax.tree.map(lambda _: pl.BlockSpec(memory_space=pltpu.VMEM), outs),
        cost_estimate=pl.CostEstimate(flops=flops, bytes_accessed=0, transcendentals=0),
        compiler_params=pltpu.CompilerParams(vmem_limit_bytes=16 << 20),
    )(*args)


def cos_sin(steps, period):
    quarter = steps.astype(jnp.float32) * (4.0 / period)
    nearest = jnp.floor(quarter + 0.5)
    angle = (quarter - nearest) * (math.pi / 2)
    square = angle * angle
    sine, cosine = SIN_TERMS[-1], COS_TERMS[-1]
    for s_term, c_term in zip(SIN_TERMS[-2::-1], COS_TERMS[-2::-1]):
        sine, cosine = sine * square + s_term, cosine * square + c_term
    sine = sine * angle
    turn = nearest.astype(jnp.int32)
    swap, low = (turn & 1) == 1, (turn & 2) == 2
    c_abs, s_abs = jnp.where(swap, sine, cosine), jnp.where(swap, cosine, sine)
    return jnp.where(swap != low, -c_abs, c_abs), jnp.where(low, -s_abs, s_abs)


def features(cycles, planes, own_ref, theta_ref, phi_ref, psi_ref, cos_ref, sin_ref, first_ref, second_ref):
    own = own_ref[0]
    modes = cos_ref.shape[0]
    halves = first_ref.shape[0]
    wide = 2 * planes
    for row in range(theta_ref.shape[0]):
        at = pl.ds(row * LANES, LANES)
        theta, phi, psi = (ref[row : row + 1, :] for ref in (theta_ref, phi_ref, psi_ref))
        step = min(modes, 2 * SUBLANES)

        def turn_phi(first, at=at, phi=phi, step=step):
            mode = first + lax.broadcasted_iota(jnp.int32, (step, LANES), 0)
            c, s = cos_sin((mode * phi) & (NPHI - 1), NPHI)
            cos_ref[pl.ds(first, step), at] = c
            sin_ref[pl.ds(first, step), at] = s

        if modes == step:
            turn_phi(0)
        else:
            pl.loop(0, modes, step=step)(turn_phi)
        for half in range(halves):
            inner = lax.broadcasted_iota(jnp.int32, (wide, LANES), 0)
            part = (own ^ (2 * half)) ^ (inner // planes)
            plane = part * planes + inner % planes
            c, s = cos_sin((plane * psi) & (NPSI - 1), NPSI)
            chosen = [theta == cycle for cycle in range(cycles)]
            cs = [jnp.where(pick, c, 0.0) for pick in chosen]
            ss = [jnp.where(pick, s, 0.0) for pick in chosen]
            for ref, rows in ((first_ref, cs + [-v for v in ss]), (second_ref, ss + cs)):
                full = jnp.concatenate(rows, axis=0)
                high = full.astype(jnp.bfloat16)
                low = (full - high.astype(jnp.float32)).astype(jnp.bfloat16)
                ref[half, :, at] = jnp.concatenate([high, high, low, jnp.zeros_like(low)], axis=0)


def cubes(masks, place_ref, near_ref, far_ref, beam_ref, beam_far_ref, table_ref, table_far_ref, out_ref):
    place = place_ref[0]
    cycles, modes, planes, band = table_ref.shape
    blocks = near_ref.shape[0]
    each = near_ref.shape[3]
    f32 = jnp.float32
    beam = [
        [jnp.concatenate([beam_ref[k, c], beam_far_ref[k, c]], axis=0).astype(f32) for c in range(beam_ref.shape[1])]
        for k in range(2)
    ]
    rows = 2 * cycles * 2 * planes

    def one_mode(mode, block, inner, total):
        sky = [
            [
                jnp.where(
                    block < blocks,
                    near_ref[block & (blocks - 1), k, c, inner : inner + 1, :],
                    far_ref[block & (blocks - 1), k, c, inner : inner + 1, :],
                ).astype(f32)
                for c in range(near_ref.shape[2])
            ]
            for k in range(2)
        ]
        real = sum(sky[0][c] * beam[0][c] - sky[1][c] * beam[1][c] for c in range(len(beam[0])))
        imag = sum(sky[0][c] * beam[1][c] + sky[1][c] * beam[0][c] for c in range(len(beam[0])))
        spectra = [v.astype(jnp.bfloat16).astype(f32) for v in (real, imag)]
        tables = [
            jnp.concatenate([table_ref[g, mode], table_far_ref[g, mode]], axis=0).astype(f32) for g in range(cycles)
        ]
        products = jnp.concatenate([s * t for s in spectra for t in tables], axis=0)
        sums = jnp.sum(products, axis=1, keepdims=True)
        lane = lax.broadcasted_iota(jnp.int32, (rows, LANES), 1)
        return jnp.where(lane == mode % LANES, sums, total)

    def block_of(owner):
        rest, block = owner ^ place, 0
        for level, mask in enumerate(masks):
            bit = (rest >> (mask.bit_length() - 1)) & 1
            rest = rest ^ (bit * mask)
            block = block | (bit << level)
        return block

    for base in range(0, modes, LANES):
        count = min(modes, LANES)
        total = jnp.zeros((rows, LANES), f32)
        if count * cycles <= LANES:
            for mode in range(base, base + count):
                total = one_mode(mode, block_of(mode // each), mode % each, total)
        else:

            def owned(owner, total):
                for inner in range(each):
                    total = one_mode(owner * each + inner, block_of(owner), inner, total)
                return total

            total = lax.fori_loop(base // each, (base + count) // each, owned, total)
        out_ref[base : base + count, :] = jnp.concatenate([total, total], axis=0).T[:count]


def sampled(cube, cos_ref, sin_ref, first, second, row):
    rows = cube.shape[1] // 2
    at = pl.ds(row * LANES, LANES)
    high = cube.astype(jnp.bfloat16)
    low = (cube - high.astype(jnp.float32)).astype(jnp.bfloat16)
    lane = lax.broadcasted_iota(jnp.int32, cube.shape, 1)
    left = jnp.concatenate([jnp.where(lane < rows, high, low), high], axis=1)
    real = jnp.dot(left, first[:, at], preferred_element_type=jnp.float32)
    imag = jnp.dot(left, second[:, at], preferred_element_type=jnp.float32)
    return jnp.sum(real * cos_ref[:, at] - imag * sin_ref[:, at], axis=0, keepdims=True)


def near_half(cube_ref, cos_ref, sin_ref, first_ref, second_ref, out_ref):
    cube = cube_ref[...]
    for row in range(out_ref.shape[0]):
        out_ref[row : row + 1, :] = sampled(cube, cos_ref, sin_ref, first_ref.at[0], second_ref.at[0], row)


def far_half(start, cube_ref, cos_ref, sin_ref, first_ref, second_ref, near_ref, out_ref):
    rows, width = near_ref.shape[0], out_ref.shape[1]
    done = []
    for row in range(rows):
        total = near_ref[row : row + 1, :]
        for half in range(cube_ref.shape[0]):
            total += sampled(
                cube_ref[half], cos_ref, sin_ref, first_ref.at[start + half], second_ref.at[start + half], row
            )
        done.append(total)
    whole = jnp.concatenate(done, axis=0)
    for part in range(LANES // width):
        out_ref[part * rows : (part + 1) * rows, :] = whole[:, part * width : (part + 1) * width]


def on_device(sky_alm, beam_blm, wigner, theta_index, phi_index, psi_index):
    f32, bf16 = jnp.float32, jnp.bfloat16
    groups, parts = lax.axis_size("det"), lax.axis_size("bm")
    place, own = lax.axis_index("det"), lax.axis_index("bm")
    cycles, modes, planes, _ = wigner.shape
    detectors = theta_index.shape[0]
    width = theta_index.shape[1] // parts
    packed = LANES // width
    samples = detectors * width

    def trade(values, axis, mask):
        return lax.ppermute(values, axis, [(i, i ^ mask) for i in range(lax.axis_size(axis))])

    masks = [(1 << level) | 1 for level in reversed(range(1, groups.bit_length() - 1))] + [1]
    near = sky_alm[None]
    far = trade(near, "det", masks[0])
    table_far = trade(wigner, "bm", 1)
    beam_far = trade(beam_blm, "bm", 1)
    for mask in masks[1:]:
        near = jnp.concatenate([near, far])
        far = trade(near, "det", mask)

    def columns(values):
        held = lax.dynamic_slice_in_dim(values, own * width, width, 1)
        return held.reshape(packed, detectors // packed, width).swapaxes(0, 1).reshape(-1, LANES)

    rows = 2 * cycles * 2 * planes
    factors = jax.ShapeDtypeStruct((parts // 2, 4 * rows, samples), bf16)
    waves = jax.ShapeDtypeStruct((modes, samples), f32)
    cosine, sine, first, second = kernel_call(
        functools.partial(features, cycles, planes),
        [waves, waves, factors, factors],
        own.reshape(1),
        columns(theta_index),
        columns(phi_index),
        columns(psi_index),
    )
    half = kernel_call(
        functools.partial(cubes, masks),
        jax.ShapeDtypeStruct((modes, 2 * rows), f32),
        place.reshape(1),
        near,
        far,
        beam_blm,
        beam_far,
        wigner,
        table_far,
    )
    held, others, bit = half[None], [], 2
    while bit < parts:
        others.append(trade(held, "bm", bit))
        if 2 * bit < parts:
            held = jnp.concatenate([held, others[-1]])
        bit *= 2
    partial = kernel_call(
        near_half, jax.ShapeDtypeStruct((samples // LANES, LANES), f32), half, cosine, sine, first, second, scalars=0
    )
    others = others[0] if len(others) == 1 else jnp.concatenate(others)
    return kernel_call(
        functools.partial(far_half, 1),
        jax.ShapeDtypeStruct((detectors, width), f32),
        others,
        cosine,
        sine,
        first,
        second,
        partial,
        scalars=0,
    )


def solution(mesh):
    placed = (
        P(None, None, "det", None),
        P(None, None, "bm", None),
        P("det", None, "bm", None),
        P("det", None),
        P("det", None),
        P("det", None),
    )
    return jax.shard_map(
        on_device, mesh=mesh, in_specs=placed, out_specs=P("det", "bm"), check_vma=False
    )
```

```python
import functools
import math

import jax
import jax.numpy as jnp
from jax import lax
from jax.experimental import pallas as pl
from jax.experimental.pallas import tpu as pltpu
from jax.sharding import PartitionSpec as P


NPHI = 16384
NPSI = 32
LANES = 128
SUBLANES = 8

SIN_TERMS = (1.0, -1 / 6, 1 / 120, -1 / 5040, 1 / 362880)
COS_TERMS = (1.0, -1 / 2, 1 / 24, -1 / 720, 1 / 40320)


def kernel_call(body, outs, *args, scalars=1, flops=0):
    spaces = [pltpu.SMEM] * scalars + [pltpu.VMEM] * (len(args) - scalars)
    return pl.pallas_call(
        body,
        out_shape=outs,
        in_specs=[pl.BlockSpec(memory_space=space) for space in spaces],
        out_specs=jax.tree.map(lambda _: pl.BlockSpec(memory_space=pltpu.VMEM), outs),
        cost_estimate=pl.CostEstimate(flops=flops, bytes_accessed=0, transcendentals=0),
        compiler_params=pltpu.CompilerParams(vmem_limit_bytes=16 << 20),
    )(*args)


def staged(sky_ref, beam_ref, table_ref, sky_out, pack_out, sems):
    rows = table_ref.shape[0]
    copies = [
        pltpu.make_async_copy(sky_ref, sky_out, sems.at[0]),
        pltpu.make_async_copy(table_ref, pack_out.at[:rows], sems.at[1]),
        pltpu.make_async_copy(beam_ref, pack_out.at[rows:], sems.at[2]),
    ]
    for copy in copies:
        copy.start()
    for copy in copies:
        copy.wait()


def cos_sin(steps, period):
    quarter = steps.astype(jnp.float32) * (4.0 / period)
    nearest = jnp.floor(quarter + 0.5)
    angle = (quarter - nearest) * (math.pi / 2)
    square = angle * angle
    sine, cosine = SIN_TERMS[-1], COS_TERMS[-1]
    for s_term, c_term in zip(SIN_TERMS[-2::-1], COS_TERMS[-2::-1]):
        sine, cosine = sine * square + s_term, cosine * square + c_term
    sine = sine * angle
    turn = nearest.astype(jnp.int32)
    swap, low = (turn & 1) == 1, (turn & 2) == 2
    c_abs, s_abs = jnp.where(swap, sine, cosine), jnp.where(swap, cosine, sine)
    return jnp.where(swap != low, -c_abs, c_abs), jnp.where(low, -s_abs, s_abs)


def features(cycles, planes, own_ref, theta_ref, phi_ref, psi_ref, cos_ref, sin_ref, first_ref, second_ref):
    own = own_ref[0]
    modes = cos_ref.shape[0]
    halves = first_ref.shape[0]
    wide = 2 * planes
    for row in range(theta_ref.shape[0]):
        at = pl.ds(row * LANES, LANES)
        theta, phi, psi = (ref[row : row + 1, :] for ref in (theta_ref, phi_ref, psi_ref))
        step = min(modes, 2 * SUBLANES)

        def turn_phi(first, at=at, phi=phi, step=step):
            mode = first + lax.broadcasted_iota(jnp.int32, (step, LANES), 0)
            c, s = cos_sin((mode * phi) & (NPHI - 1), NPHI)
            cos_ref[pl.ds(first, step), at] = c
            sin_ref[pl.ds(first, step), at] = s

        if modes == step:
            turn_phi(0)
        else:
            pl.loop(0, modes, step=step)(turn_phi)
        for half in range(halves):
            inner = lax.broadcasted_iota(jnp.int32, (wide, LANES), 0)
            part = (own ^ (2 * half)) ^ (inner // planes)
            plane = part * planes + inner % planes
            c, s = cos_sin((plane * psi) & (NPSI - 1), NPSI)
            chosen = [theta == cycle for cycle in range(cycles)]
            cs = [jnp.where(pick, c, 0.0) for pick in chosen]
            ss = [jnp.where(pick, s, 0.0) for pick in chosen]
            for ref, rows in ((first_ref, cs + [-v for v in ss]), (second_ref, ss + cs)):
                full = jnp.concatenate(rows, axis=0)
                high = full.astype(jnp.bfloat16)
                low = (full - high.astype(jnp.float32)).astype(jnp.bfloat16)
                ref[half, :, at] = jnp.concatenate([high, high, low, jnp.zeros_like(low)], axis=0)


def cubes(masks, cycles, place_ref, near_ref, far_ref, pack_ref, pack_far_ref, out_ref):
    place = place_ref[0]
    modes = out_ref.shape[0]
    planes = pack_ref.shape[1]
    blocks, kinds, each = near_ref.shape[0], near_ref.shape[2], near_ref.shape[3]
    f32 = jnp.float32

    def both(row):
        return jnp.concatenate([pack_ref[row], pack_far_ref[row]], axis=0).astype(f32)

    beam = [[both(cycles * modes + k * kinds + c) for c in range(kinds)] for k in range(2)]
    rows = 2 * cycles * 2 * planes

    def one_mode(mode, block, inner, total):
        sky = [
            [
                jnp.where(
                    block < blocks,
                    near_ref[block & (blocks - 1), k, c, inner : inner + 1, :],
                    far_ref[block & (blocks - 1), k, c, inner : inner + 1, :],
                ).astype(f32)
                for c in range(kinds)
            ]
            for k in range(2)
        ]
        real = sum(sky[0][c] * beam[0][c] - sky[1][c] * beam[1][c] for c in range(kinds))
        imag = sum(sky[0][c] * beam[1][c] + sky[1][c] * beam[0][c] for c in range(kinds))
        spectra = [v.astype(jnp.bfloat16).astype(f32) for v in (real, imag)]
        tables = [both(g * modes + mode) for g in range(cycles)]
        products = jnp.concatenate([s * t for s in spectra for t in tables], axis=0)
        sums = jnp.sum(products, axis=1, keepdims=True)
        lane = lax.broadcasted_iota(jnp.int32, (rows, LANES), 1)
        return jnp.where(lane == mode % LANES, sums, total)

    def block_of(owner):
        rest, block = owner ^ place, 0
        for level, mask in enumerate(masks):
            bit = (rest >> (mask.bit_length() - 1)) & 1
            rest = rest ^ (bit * mask)
            block = block | (bit << level)
        return block

    for base in range(0, modes, LANES):
        count = min(modes, LANES)
        total = jnp.zeros((rows, LANES), f32)
        if count * cycles <= LANES:
            for mode in range(base, base + count):
                total = one_mode(mode, block_of(mode // each), mode % each, total)
        else:

            def owned(owner, total):
                for inner in range(each):
                    total = one_mode(owner * each + inner, block_of(owner), inner, total)
                return total

            total = lax.fori_loop(base // each, (base + count) // each, owned, total)
        out_ref[base : base + count, :] = jnp.concatenate([total, total], axis=0).T[:count]


def sampled(cube, cos_ref, sin_ref, first, second, row):
    rows = cube.shape[1] // 2
    at = pl.ds(row * LANES, LANES)
    high = cube.astype(jnp.bfloat16)
    low = (cube - high.astype(jnp.float32)).astype(jnp.bfloat16)
    lane = lax.broadcasted_iota(jnp.int32, cube.shape, 1)
    left = jnp.concatenate([jnp.where(lane < rows, high, low), high], axis=1)
    real = jnp.dot(left, first[:, at], preferred_element_type=jnp.float32)
    imag = jnp.dot(left, second[:, at], preferred_element_type=jnp.float32)
    return jnp.sum(real * cos_ref[:, at] - imag * sin_ref[:, at], axis=0, keepdims=True)


def near_half(cube_ref, cos_ref, sin_ref, first_ref, second_ref, out_ref):
    cube = cube_ref[...]
    for row in range(out_ref.shape[0]):
        out_ref[row : row + 1, :] = sampled(cube, cos_ref, sin_ref, first_ref.at[0], second_ref.at[0], row)


def far_half(start, cube_ref, cos_ref, sin_ref, first_ref, second_ref, near_ref, out_ref):
    rows, width = near_ref.shape[0], out_ref.shape[1]
    done = []
    for row in range(rows):
        total = near_ref[row : row + 1, :]
        for half in range(cube_ref.shape[0]):
            total += sampled(
                cube_ref[half], cos_ref, sin_ref, first_ref.at[start + half], second_ref.at[start + half], row
            )
        done.append(total)
    whole = jnp.concatenate(done, axis=0)
    for part in range(LANES // width):
        out_ref[part * rows : (part + 1) * rows, :] = whole[:, part * width : (part + 1) * width]


def on_device(sky_alm, beam_blm, wigner, theta_index, phi_index, psi_index):
    f32, bf16 = jnp.float32, jnp.bfloat16
    groups, parts = lax.axis_size("det"), lax.axis_size("bm")
    place, own = lax.axis_index("det"), lax.axis_index("bm")
    cycles, modes, planes, _ = wigner.shape
    detectors = theta_index.shape[0]
    width = theta_index.shape[1] // parts
    packed = LANES // width
    samples = detectors * width

    def in_hbm(values):
        return pltpu.with_memory_space_constraint(values, pltpu.HBM)

    def trade(values, axis, mask):
        return lax.ppermute(values, axis, [(i, i ^ mask) for i in range(lax.axis_size(axis))])

    sky, pack = pl.pallas_call(
        staged,
        out_shape=[
            jax.ShapeDtypeStruct((1,) + sky_alm.shape, bf16),
            jax.ShapeDtypeStruct((cycles * modes + 2 * beam_blm.shape[1],) + wigner.shape[2:], bf16),
        ],
        in_specs=[pl.BlockSpec(memory_space=pltpu.HBM)] * 3,
        out_specs=[pl.BlockSpec(memory_space=pltpu.VMEM)] * 2,
        scratch_shapes=[pltpu.SemaphoreType.DMA((3,))],
        compiler_params=pltpu.CompilerParams(vmem_limit_bytes=16 << 20),
    )(
        in_hbm(sky_alm[None]),
        in_hbm(beam_blm.reshape((-1,) + beam_blm.shape[2:])),
        in_hbm(wigner.reshape((-1,) + wigner.shape[2:])),
    )
    masks = [(1 << level) | 1 for level in reversed(range(1, groups.bit_length() - 1))] + [1]
    near = sky
    far = trade(near, "det", masks[0])
    pack_far = trade(pack, "bm", 1)
    for mask in masks[1:]:
        near = jnp.concatenate([near, far])
        far = trade(near, "det", mask)

    def columns(values):
        held = lax.dynamic_slice_in_dim(values, own * width, width, 1)
        return held.reshape(packed, detectors // packed, width).swapaxes(0, 1).reshape(-1, LANES)

    rows = 2 * cycles * 2 * planes
    factors = jax.ShapeDtypeStruct((parts // 2, 4 * rows, samples), bf16)
    waves = jax.ShapeDtypeStruct((modes, samples), f32)
    cosine, sine, first, second = kernel_call(
        functools.partial(features, cycles, planes),
        [waves, waves, factors, factors],
        own.reshape(1),
        columns(theta_index),
        columns(phi_index),
        columns(psi_index),
    )
    half = kernel_call(
        functools.partial(cubes, masks, cycles),
        jax.ShapeDtypeStruct((modes, 2 * rows), f32),
        place.reshape(1),
        near,
        far,
        pack,
        pack_far,
    )
    held, others, bit = half[None], [], 2
    while bit < parts:
        others.append(trade(held, "bm", bit))
        if 2 * bit < parts:
            held = jnp.concatenate([held, others[-1]])
        bit *= 2
    partial = kernel_call(
        near_half, jax.ShapeDtypeStruct((samples // LANES, LANES), f32), half, cosine, sine, first, second, scalars=0
    )
    others = others[0] if len(others) == 1 else jnp.concatenate(others)
    return kernel_call(
        functools.partial(far_half, 1),
        jax.ShapeDtypeStruct((detectors, width), f32),
        others,
        cosine,
        sine,
        first,
        second,
        partial,
        scalars=0,
    )


def solution(mesh):
    placed = (
        P(None, None, "det", None),
        P(None, None, "bm", None),
        P("det", None, "bm", None),
        P("det", None),
        P("det", None),
        P("det", None),
    )
    return jax.shard_map(
        on_device, mesh=mesh, in_specs=placed, out_specs=P("det", "bm"), check_vma=False
    )
```

```python
import functools
import math

import jax
import jax.numpy as jnp
from jax import lax
from jax.experimental import pallas as pl
from jax.experimental.pallas import tpu as pltpu
from jax.sharding import PartitionSpec as P


NPHI = 16384
NPSI = 32
LANES = 128
SUBLANES = 8

SIN_TERMS = (1.0, -1 / 6, 1 / 120, -1 / 5040, 1 / 362880)
COS_TERMS = (1.0, -1 / 2, 1 / 24, -1 / 720, 1 / 40320)


def kernel_call(body, outs, *args, scalars=1, flops=0, scratch=()):
    spaces = [pltpu.SMEM] * scalars + [pltpu.VMEM] * (len(args) - scalars)
    return pl.pallas_call(
        body,
        out_shape=outs,
        in_specs=[pl.BlockSpec(memory_space=space) for space in spaces],
        out_specs=jax.tree.map(lambda _: pl.BlockSpec(memory_space=pltpu.VMEM), outs),
        scratch_shapes=list(scratch),
        cost_estimate=pl.CostEstimate(flops=flops, bytes_accessed=0, transcendentals=0),
        compiler_params=pltpu.CompilerParams(vmem_limit_bytes=16 << 20),
    )(*args)


def staged(*refs):
    *given, out_ref, sems = refs
    copies, start = [], 0
    for i, ref in enumerate(given):
        stop = start + ref.shape[0]
        copies.append(pltpu.make_async_copy(ref, out_ref.at[start:stop], sems.at[i]))
        start = stop
    for copy in copies:
        copy.start()
    for copy in copies:
        copy.wait()


def cos_sin(steps, period):
    quarter = steps.astype(jnp.float32) * (4.0 / period)
    nearest = jnp.floor(quarter + 0.5)
    angle = (quarter - nearest) * (math.pi / 2)
    square = angle * angle
    sine, cosine = SIN_TERMS[-1], COS_TERMS[-1]
    for s_term, c_term in zip(SIN_TERMS[-2::-1], COS_TERMS[-2::-1]):
        sine, cosine = sine * square + s_term, cosine * square + c_term
    sine = sine * angle
    turn = nearest.astype(jnp.int32)
    swap, low = (turn & 1) == 1, (turn & 2) == 2
    c_abs, s_abs = jnp.where(swap, sine, cosine), jnp.where(swap, cosine, sine)
    return jnp.where(swap != low, -c_abs, c_abs), jnp.where(low, -s_abs, s_abs)


def own_samples(ref, own, width):
    values = pltpu.roll(ref[...], lax.rem(ref.shape[1] - own * width, ref.shape[1]), 1)[:, :LANES]
    packed = LANES // width
    rows = ref.shape[0] // packed
    lane = lax.broadcasted_iota(jnp.int32, (rows, LANES), 1)
    held = values[:rows]
    for part in range(1, packed):
        moved = pltpu.roll(values[part * rows : (part + 1) * rows], part * width, 1)
        held = jnp.where(lane // width == part, moved, held)
    return held


def features(cycles, planes, width, own_ref, theta_ref, phi_ref, psi_ref, cos_ref, sin_ref, first_ref, second_ref):
    own = own_ref[0]
    modes = cos_ref.shape[0]
    halves = first_ref.shape[0]
    wide = 2 * planes
    thetas, phis, psis = (own_samples(ref, own, width) for ref in (theta_ref, phi_ref, psi_ref))
    for row in range(thetas.shape[0]):
        at = pl.ds(row * LANES, LANES)
        theta, phi, psi = (values[row : row + 1] for values in (thetas, phis, psis))
        step = min(modes, 2 * SUBLANES)

        def turn_phi(first, at=at, phi=phi, step=step):
            mode = first + lax.broadcasted_iota(jnp.int32, (step, LANES), 0)
            c, s = cos_sin((mode * phi) & (NPHI - 1), NPHI)
            cos_ref[pl.ds(first, step), at] = c
            sin_ref[pl.ds(first, step), at] = s

        if modes == step:
            turn_phi(0)
        else:
            pl.loop(0, modes, step=step)(turn_phi)
        for half in range(halves):
            inner = lax.broadcasted_iota(jnp.int32, (wide, LANES), 0)
            part = (own ^ (2 * half)) ^ (inner // planes)
            plane = part * planes + inner % planes
            c, s = cos_sin((plane * psi) & (NPSI - 1), NPSI)
            chosen = [theta == cycle for cycle in range(cycles)]
            cs = [jnp.where(pick, c, 0.0) for pick in chosen]
            ss = [jnp.where(pick, s, 0.0) for pick in chosen]
            for ref, rows in ((first_ref, cs + [-v for v in ss]), (second_ref, ss + cs)):
                full = jnp.concatenate(rows, axis=0)
                high = full.astype(jnp.bfloat16)
                low = (full - high.astype(jnp.float32)).astype(jnp.bfloat16)
                ref[half, :, at] = jnp.concatenate([high, high, low, jnp.zeros_like(low)], axis=0)


def cubes(masks, cycles, place_ref, held_ref, b_ref, a_ref, c_ref, pack_ref, pack_far_ref, out_ref, sky_ref):
    place = place_ref[0]
    modes = out_ref.shape[0]
    planes = pack_ref.shape[1]
    blocks, kinds, each = held_ref.shape[0], held_ref.shape[2], held_ref.shape[3]
    f32 = jnp.float32
    for i, ref in enumerate((held_ref, b_ref, a_ref, c_ref)):
        sky_ref[i * blocks : (i + 1) * blocks] = ref[...]

    def both(row):
        return jnp.concatenate([pack_ref[row], pack_far_ref[row]], axis=0).astype(f32)

    beam = [[both(cycles * modes + k * kinds + c) for c in range(kinds)] for k in range(2)]
    rows = 2 * cycles * 2 * planes

    def one_mode(mode, block, inner, total):
        sky = [[sky_ref[block, k, c, inner : inner + 1, :].astype(f32) for c in range(kinds)] for k in range(2)]
        real = sum(sky[0][c] * beam[0][c] - sky[1][c] * beam[1][c] for c in range(kinds))
        imag = sum(sky[0][c] * beam[1][c] + sky[1][c] * beam[0][c] for c in range(kinds))
        spectra = [v.astype(jnp.bfloat16).astype(f32) for v in (real, imag)]
        tables = [both(g * modes + mode) for g in range(cycles)]
        products = jnp.concatenate([s * t for s in spectra for t in tables], axis=0)
        sums = jnp.sum(products, axis=1, keepdims=True)
        lane = lax.broadcasted_iota(jnp.int32, (rows, LANES), 1)
        return jnp.where(lane == mode % LANES, sums, total)

    def block_of(owner):
        rest, odd = owner ^ place, place & 1
        low, high = (rest >> 1) & 1, (rest >> 2) & 1
        crossed = odd ^ low
        arrived = jnp.where(crossed == 0, jnp.where(odd == 0, 4, 6), jnp.where(odd == 0, 7, 5))
        rest = rest ^ jnp.where(high == 1, arrived, 3 * low)
        source = jnp.where(high == 1, 2 + crossed, low)
        block = rest & 1
        for level, mask in enumerate(masks):
            bit = (rest >> (mask.bit_length() - 1)) & 1
            block = (block ^ bit) | (bit << (level + 1))
        return source * blocks + block

    for base in range(0, modes, LANES):
        count = min(modes, LANES)
        total = jnp.zeros((rows, LANES), f32)
        if count * cycles <= LANES:
            for mode in range(base, base + count):
                total = one_mode(mode, block_of(mode // each), mode % each, total)
        else:

            def owned(owner, total):
                for inner in range(each):
                    total = one_mode(owner * each + inner, block_of(owner), inner, total)
                return total

            total = lax.fori_loop(base // each, (base + count) // each, owned, total)
        out_ref[base : base + count, :] = jnp.concatenate([total, total], axis=0).T[:count]


def sampled(cube, cos_ref, sin_ref, first, second, row):
    rows = cube.shape[1] // 2
    at = pl.ds(row * LANES, LANES)
    high = cube.astype(jnp.bfloat16)
    low = (cube - high.astype(jnp.float32)).astype(jnp.bfloat16)
    lane = lax.broadcasted_iota(jnp.int32, cube.shape, 1)
    left = jnp.concatenate([jnp.where(lane < rows, high, low), high], axis=1)
    real = jnp.dot(left, first[:, at], preferred_element_type=jnp.float32)
    imag = jnp.dot(left, second[:, at], preferred_element_type=jnp.float32)
    return jnp.sum(real * cos_ref[:, at] - imag * sin_ref[:, at], axis=0, keepdims=True)


def near_half(cube_ref, cos_ref, sin_ref, first_ref, second_ref, out_ref):
    cube = cube_ref[...]
    for row in range(out_ref.shape[0]):
        out_ref[row : row + 1, :] = sampled(cube, cos_ref, sin_ref, first_ref.at[0], second_ref.at[0], row)


def far_half(start, cube_ref, cos_ref, sin_ref, first_ref, second_ref, near_ref, out_ref):
    rows, width = near_ref.shape[0], out_ref.shape[1]
    done = []
    for row in range(rows):
        total = near_ref[row : row + 1, :]
        for half in range(cube_ref.shape[0]):
            total += sampled(
                cube_ref[half], cos_ref, sin_ref, first_ref.at[start + half], second_ref.at[start + half], row
            )
        done.append(total)
    whole = jnp.concatenate(done, axis=0)
    for part in range(LANES // width):
        out_ref[part * rows : (part + 1) * rows, :] = whole[:, part * width : (part + 1) * width]


def on_device(sky_alm, beam_blm, wigner, theta_index, phi_index, psi_index):
    f32, bf16 = jnp.float32, jnp.bfloat16
    groups, parts = lax.axis_size("det"), lax.axis_size("bm")
    place, own = lax.axis_index("det"), lax.axis_index("bm")
    cycles, modes, planes, _ = wigner.shape
    detectors = theta_index.shape[0]
    width = theta_index.shape[1] // parts
    samples = detectors * width

    def in_hbm(values):
        return pltpu.with_memory_space_constraint(values, pltpu.HBM)

    def trade(values, det_mask, bm_mask=0, odd_mask=None):
        pairs = []
        for i in range(groups):
            mask = odd_mask if odd_mask is not None and i % 2 else det_mask
            pairs += [(i * parts + j, (i ^ mask) * parts + (j ^ bm_mask)) for j in range(parts)]
        return lax.ppermute(values, ("det", "bm"), pairs)

    given = [values.reshape((-1,) + wigner.shape[2:]) for values in (wigner, beam_blm, sky_alm)]
    length = sum(values.shape[0] for values in given)
    pack = pl.pallas_call(
        staged,
        out_shape=jax.ShapeDtypeStruct((length,) + wigner.shape[2:], bf16),
        in_specs=[pl.BlockSpec(memory_space=pltpu.HBM)] * 3,
        out_specs=pl.BlockSpec(memory_space=pltpu.VMEM),
        scratch_shapes=[pltpu.SemaphoreType.DMA((3,))],
        compiler_params=pltpu.CompilerParams(vmem_limit_bytes=16 << 20),
    )(*[in_hbm(values) for values in given])

    def sky_of(values):
        return values[length - given[2].shape[0] :].reshape((1,) + sky_alm.shape)

    pack_near = trade(pack, 1)
    pack_far = trade(pack, 1, 1)
    held = jnp.concatenate([sky_of(pack), sky_of(pack_near)])
    masks = [(1 << level) | 1 for level in range(3, groups.bit_length() - 1)]
    for mask in masks:
        held = jnp.concatenate([held, trade(held, mask)])
    sky_a = trade(held, 4, odd_mask=6)
    sky_b = trade(held, 3)
    sky_c = trade(sky_a, 1)

    rows = 2 * cycles * 2 * planes
    factors = jax.ShapeDtypeStruct((parts // 2, 4 * rows, samples), bf16)
    waves = jax.ShapeDtypeStruct((modes, samples), f32)
    cosine, sine, first, second = kernel_call(
        functools.partial(features, cycles, planes, width),
        [waves, waves, factors, factors],
        own.reshape(1),
        theta_index,
        phi_index,
        psi_index,
    )
    half = kernel_call(
        functools.partial(cubes, masks, cycles),
        jax.ShapeDtypeStruct((modes, 2 * rows), f32),
        place.reshape(1),
        held,
        sky_b,
        sky_a,
        sky_c,
        pack_near,
        pack_far,
        scratch=[pltpu.VMEM((groups,) + sky_alm.shape, bf16)],
    )
    far = trade(half, 1, 2)[None]
    near = trade(half, 1)
    bit = 4
    while bit < parts:
        far = jnp.concatenate([far, trade(jnp.concatenate([near[None], far]), 0, bit)])
        bit *= 2
    partial = kernel_call(
        near_half, jax.ShapeDtypeStruct((samples // LANES, LANES), f32), near, cosine, sine, first, second, scalars=0
    )
    return kernel_call(
        functools.partial(far_half, 1),
        jax.ShapeDtypeStruct((detectors, width), f32),
        far,
        cosine,
        sine,
        first,
        second,
        partial,
        scalars=0,
    )


def solution(mesh):
    placed = (
        P(None, None, "det", None),
        P(None, None, "bm", None),
        P("det", None, "bm", None),
        P("det", None),
        P("det", None),
        P("det", None),
    )
    return jax.shard_map(
        on_device, mesh=mesh, in_specs=placed, out_specs=P("det", "bm"), check_vma=False
    )
```

```python
import functools
import math

import jax
import jax.numpy as jnp
from jax import lax
from jax.experimental import pallas as pl
from jax.experimental.pallas import tpu as pltpu
from jax.sharding import PartitionSpec as P


NPHI = 16384
NPSI = 32
LANES = 128
SUBLANES = 8

SIN_TERMS = (1.0, -1 / 6, 1 / 120, -1 / 5040, 1 / 362880)
COS_TERMS = (1.0, -1 / 2, 1 / 24, -1 / 720, 1 / 40320)


def kernel_call(body, outs, *args, scalars=1, flops=0, scratch=()):
    spaces = [pltpu.SMEM] * scalars + [pltpu.VMEM] * (len(args) - scalars)
    return pl.pallas_call(
        body,
        out_shape=outs,
        in_specs=[pl.BlockSpec(memory_space=space) for space in spaces],
        out_specs=jax.tree.map(lambda _: pl.BlockSpec(memory_space=pltpu.VMEM), outs),
        scratch_shapes=list(scratch),
        cost_estimate=pl.CostEstimate(flops=flops, bytes_accessed=0, transcendentals=0),
        compiler_params=pltpu.CompilerParams(vmem_limit_bytes=16 << 20),
    )(*args)


def staged(*refs):
    *given, out_ref, sems = refs
    copies, start = [], 0
    for i, ref in enumerate(given):
        stop = start + ref.shape[0]
        copies.append(pltpu.make_async_copy(ref, out_ref.at[start:stop], sems.at[i]))
        start = stop
    for copy in copies:
        copy.start()
    for copy in copies:
        copy.wait()


def cos_sin(steps, period):
    quarter = steps.astype(jnp.float32) * (4.0 / period)
    nearest = jnp.floor(quarter + 0.5)
    angle = (quarter - nearest) * (math.pi / 2)
    square = angle * angle
    sine, cosine = SIN_TERMS[-1], COS_TERMS[-1]
    for s_term, c_term in zip(SIN_TERMS[-2::-1], COS_TERMS[-2::-1]):
        sine, cosine = sine * square + s_term, cosine * square + c_term
    sine = sine * angle
    turn = nearest.astype(jnp.int32)
    swap, low = (turn & 1) == 1, (turn & 2) == 2
    c_abs, s_abs = jnp.where(swap, sine, cosine), jnp.where(swap, cosine, sine)
    return jnp.where(swap != low, -c_abs, c_abs), jnp.where(low, -s_abs, s_abs)


def own_samples(ref, own, width):
    values = pltpu.roll(ref[...], lax.rem(ref.shape[1] - own * width, ref.shape[1]), 1)[:, :LANES]
    packed = LANES // width
    rows = ref.shape[0] // packed
    lane = lax.broadcasted_iota(jnp.int32, (rows, LANES), 1)
    held = values[:rows]
    for part in range(1, packed):
        moved = pltpu.roll(values[part * rows : (part + 1) * rows], part * width, 1)
        held = jnp.where(lane // width == part, moved, held)
    return held


def features(cycles, planes, width, own_ref, theta_ref, phi_ref, psi_ref, cos_ref, sin_ref, factor_ref):
    own = own_ref[0]
    modes = cos_ref.shape[0]
    wide = 2 * planes
    halves = factor_ref.shape[0] // (4 * cycles * wide)
    thetas, phis, psis = (own_samples(ref, own, width) for ref in (theta_ref, phi_ref, psi_ref))
    for row in range(thetas.shape[0]):
        at = pl.ds(row * LANES, LANES)
        theta, phi, psi = (values[row : row + 1] for values in (thetas, phis, psis))
        step = min(modes, 2 * SUBLANES)

        def turn_phi(first, at=at, phi=phi, step=step):
            mode = first + lax.broadcasted_iota(jnp.int32, (step, LANES), 0)
            c, s = cos_sin((mode * phi) & (NPHI - 1), NPHI)
            cos_ref[pl.ds(first, step), at] = c
            sin_ref[pl.ds(first, step), at] = s

        if modes == step:
            turn_phi(0)
        else:
            pl.loop(0, modes, step=step)(turn_phi)
        chosen = [theta == cycle for cycle in range(cycles)]
        firsts, seconds = [], []
        for half in range(halves):
            inner = lax.broadcasted_iota(jnp.int32, (wide, LANES), 0)
            part = (own ^ (2 * half)) ^ (inner // planes)
            plane = part * planes + inner % planes
            c, s = cos_sin((plane * psi) & (NPSI - 1), NPSI)
            for pick in chosen:
                c_own, s_own = jnp.where(pick, c, 0.0), jnp.where(pick, s, 0.0)
                firsts += [c_own, -s_own]
                seconds += [s_own, c_own]
        for i, rows in enumerate((firsts, seconds)):
            full = jnp.concatenate(rows, axis=0)
            high = full.astype(jnp.bfloat16)
            low = (full - high.astype(jnp.float32)).astype(jnp.bfloat16)
            factor_ref[:, pl.ds((2 * row + i) * LANES, LANES)] = jnp.concatenate([high, low], axis=0)


def cubes(masks, shape, sources, place_ref, pack_ref, pack_far_ref, *refs):
    cycles, modes, planes = shape
    *refs, out_ref = refs
    place = place_ref[0]
    blocks, kinds, each = refs[0].shape[0], refs[0].shape[2], refs[0].shape[3]
    rows, width = 2 * cycles * 2 * planes, max(modes, LANES)
    f32 = jnp.float32
    lane = lax.broadcasted_iota(jnp.int32, (rows, width), 1)

    def both(row):
        return jnp.concatenate([pack_ref[row], pack_far_ref[row]], axis=0).astype(f32)

    beam = [[both(cycles * modes + k * kinds + c) for c in range(kinds)] for k in range(2)]

    def one_mode(mode, sky, total):
        real = sum(sky[0][c] * beam[0][c] - sky[1][c] * beam[1][c] for c in range(kinds))
        imag = sum(sky[0][c] * beam[1][c] + sky[1][c] * beam[0][c] for c in range(kinds))
        spectra = [v.astype(jnp.bfloat16).astype(f32) for v in (real, imag)]
        tables = [both(g * modes + mode) for g in range(cycles)]
        products = jnp.concatenate([s * t for t in tables for s in spectra], axis=0)
        return jnp.where(lane == mode, jnp.sum(products, axis=1, keepdims=True), total)

    def one_block(ref, sender, block, total):
        owner = sender ^ (block & 1)
        for level, mask in enumerate(masks):
            owner = owner ^ (((block >> (level + 1)) & 1) * mask)
        for inner in range(each):
            sky = [[ref[block, k, c, inner : inner + 1, :].astype(f32) for c in range(kinds)] for k in range(2)]
            total = one_mode(owner * each + inner, sky, total)
        return total

    total = refs[-1][...] if len(refs) > len(sources) else jnp.zeros((rows, width), f32)
    for ref, (even, odd) in zip(refs, sources):
        sender = place ^ jnp.where(place & 1 == 1, odd, even)
        if blocks <= SUBLANES:
            for block in range(blocks):
                total = one_block(ref, sender, block, total)
        else:
            total = lax.fori_loop(0, blocks, functools.partial(one_block, ref, sender), total)
    if out_ref.shape[0] == modes:
        for base in range(0, width, LANES):
            part = total[:, base : base + LANES]
            count = min(modes - base, LANES)
            out_ref[base : base + count, :] = jnp.concatenate([part, part], axis=0).T[:count]
    else:
        out_ref[...] = total


def sampled(near_ref, far_ref, cos_ref, sin_ref, factor_ref, out_ref):
    width = out_ref.shape[1]
    halves = [ref[half] for ref in (near_ref, far_ref) for half in range(ref.shape[0])]
    modes, doubled = halves[0].shape
    lane = lax.broadcasted_iota(jnp.int32, (modes, doubled), 1)
    whole = [jnp.where(lane < doubled // 2, *halves[i : i + 2]) for i in range(0, len(halves), 2)]
    high = [v.astype(jnp.bfloat16) for v in whole]
    low = [(v - h.astype(jnp.float32)).astype(jnp.bfloat16) for v, h in zip(whole, high)]
    left = jnp.concatenate(
        [jnp.concatenate(high + high, axis=1), jnp.concatenate(low + [jnp.zeros_like(v) for v in low], axis=1)], axis=0
    )
    done = []
    for row in range(out_ref.shape[0] * width // LANES):
        at = pl.ds(row * LANES, LANES)
        both = jnp.dot(left, factor_ref[:, pl.ds(2 * row * LANES, 2 * LANES)], preferred_element_type=jnp.float32)
        both = both[:modes] + both[modes:]
        done.append(jnp.sum(both[:, :LANES] * cos_ref[:, at] - both[:, LANES:] * sin_ref[:, at], axis=0, keepdims=True))
    result = jnp.concatenate(done, axis=0)
    rows = result.shape[0]
    for part in range(LANES // width):
        out_ref[part * rows : (part + 1) * rows, :] = result[:, part * width : (part + 1) * width]


def on_device(sky_alm, beam_blm, wigner, theta_index, phi_index, psi_index):
    f32, bf16 = jnp.float32, jnp.bfloat16
    groups, parts = lax.axis_size("det"), lax.axis_size("bm")
    place, own = lax.axis_index("det"), lax.axis_index("bm")
    cycles, modes, planes, _ = wigner.shape
    detectors = theta_index.shape[0]
    width = theta_index.shape[1] // parts
    samples = detectors * width

    def in_hbm(values):
        return pltpu.with_memory_space_constraint(values, pltpu.HBM)

    def trade(values, det_mask, bm_mask=0, odd_mask=None):
        pairs = []
        for i in range(groups):
            mask = odd_mask if odd_mask is not None and i % 2 else det_mask
            pairs += [(i * parts + j, (i ^ mask) * parts + (j ^ bm_mask)) for j in range(parts)]
        return lax.ppermute(values, ("det", "bm"), pairs)

    given = [values.reshape((-1,) + wigner.shape[2:]) for values in (wigner, beam_blm, sky_alm)]
    length = sum(values.shape[0] for values in given)
    pack = pl.pallas_call(
        staged,
        out_shape=jax.ShapeDtypeStruct((length,) + wigner.shape[2:], bf16),
        in_specs=[pl.BlockSpec(memory_space=pltpu.HBM)] * 3,
        out_specs=pl.BlockSpec(memory_space=pltpu.VMEM),
        scratch_shapes=[pltpu.SemaphoreType.DMA((3,))],
        compiler_params=pltpu.CompilerParams(vmem_limit_bytes=16 << 20),
    )(*[in_hbm(values) for values in given])

    def sky_of(values):
        return values[length - given[2].shape[0] :].reshape((1,) + sky_alm.shape)

    pack_near = trade(pack, 1)
    pack_far = trade(pack, 1, 1)
    held = jnp.concatenate([sky_of(pack), sky_of(pack_near)])
    masks = [(1 << level) | 1 for level in range(3, groups.bit_length() - 1)]
    for mask in masks:
        held = jnp.concatenate([held, trade(held, mask)])
    sky_a = trade(held, 4, odd_mask=6)
    sky_b = trade(held, 3)
    sky_c = trade(sky_a, 1)

    rows = 2 * cycles * 2 * planes
    factors = jax.ShapeDtypeStruct((2 * parts // 2 * rows, 2 * samples), bf16)
    waves = jax.ShapeDtypeStruct((modes, samples), f32)
    factors_of = kernel_call(
        functools.partial(features, cycles, planes, width),
        [waves, waves, factors],
        own.reshape(1),
        theta_index,
        phi_index,
        psi_index,
    )

    def half_cube(outs, sources, *skies):
        return kernel_call(
            functools.partial(cubes, masks, (cycles, modes, planes), sources), outs, place.reshape(1), pack_near, pack_far, *skies
        )

    columns = jax.ShapeDtypeStruct((rows, max(modes, LANES)), f32)
    half = half_cube(columns, ((0, 0), (4, 6)), held, sky_a)
    half = half_cube(jax.ShapeDtypeStruct((modes, 2 * rows), f32), ((3, 3), (7, 5)), sky_b, sky_c, half)
    far = trade(half, 1, 2)[None]
    near = trade(half, 1)[None]
    bit = 4
    while bit < parts:
        far = jnp.concatenate([far, trade(jnp.concatenate([near, far]), 0, bit)])
        bit *= 2
    return kernel_call(
        sampled,
        jax.ShapeDtypeStruct((detectors, width), f32),
        near,
        far,
        *factors_of,
        scalars=0,
    )


def solution(mesh):
    placed = (
        P(None, None, "det", None),
        P(None, None, "bm", None),
        P("det", None, "bm", None),
        P("det", None),
        P("det", None),
        P("det", None),
    )
    return jax.shard_map(
        on_device, mesh=mesh, in_specs=placed, out_specs=P("det", "bm"), check_vma=False
    )
```

```python
import functools
import math

import jax
import jax.numpy as jnp
from jax import lax
from jax.experimental import pallas as pl
from jax.experimental.pallas import tpu as pltpu
from jax.sharding import PartitionSpec as P


NPHI = 16384
NPSI = 32
LANES = 128
SUBLANES = 8

SIN_TERMS = (1.0, -1 / 6, 1 / 120, -1 / 5040, 1 / 362880)
COS_TERMS = (1.0, -1 / 2, 1 / 24, -1 / 720, 1 / 40320)


def kernel_call(body, outs, *args, scalars=1, flops=0, scratch=()):
    spaces = [pltpu.SMEM] * scalars + [pltpu.VMEM] * (len(args) - scalars)
    return pl.pallas_call(
        body,
        out_shape=outs,
        in_specs=[pl.BlockSpec(memory_space=space) for space in spaces],
        out_specs=jax.tree.map(lambda _: pl.BlockSpec(memory_space=pltpu.VMEM), outs),
        scratch_shapes=list(scratch),
        cost_estimate=pl.CostEstimate(flops=flops, bytes_accessed=0, transcendentals=0),
        compiler_params=pltpu.CompilerParams(vmem_limit_bytes=16 << 20),
    )(*args)


def joined(near_ref, far_ref, out_ref):
    rows = near_ref.shape[0]
    out_ref[:rows] = near_ref[...]
    out_ref[rows:] = far_ref[...]


def cos_sin(steps, period):
    quarter = steps.astype(jnp.float32) * (4.0 / period)
    nearest = jnp.floor(quarter + 0.5)
    angle = (quarter - nearest) * (math.pi / 2)
    square = angle * angle
    sine, cosine = SIN_TERMS[-1], COS_TERMS[-1]
    for s_term, c_term in zip(SIN_TERMS[-2::-1], COS_TERMS[-2::-1]):
        sine, cosine = sine * square + s_term, cosine * square + c_term
    sine = sine * angle
    turn = nearest.astype(jnp.int32)
    swap, low = (turn & 1) == 1, (turn & 2) == 2
    c_abs, s_abs = jnp.where(swap, sine, cosine), jnp.where(swap, cosine, sine)
    return jnp.where(swap != low, -c_abs, c_abs), jnp.where(low, -s_abs, s_abs)


def own_samples(ref, own, width):
    values = pltpu.roll(ref[...], lax.rem(ref.shape[1] - own * width, ref.shape[1]), 1)[:, :LANES]
    packed = LANES // width
    rows = ref.shape[0] // packed
    lane = lax.broadcasted_iota(jnp.int32, (rows, LANES), 1)
    held = values[:rows]
    for part in range(1, packed):
        moved = pltpu.roll(values[part * rows : (part + 1) * rows], part * width, 1)
        held = jnp.where(lane // width == part, moved, held)
    return held


def plane_rows(planes, own_ref, out_ref):
    row = lax.broadcasted_iota(jnp.int32, out_ref.shape, 0)
    out_ref[...] = (own_ref[0] ^ (row // planes)) * planes + row % planes


def features(cycles, planes, width, own_ref, theta_ref, phi_ref, psi_ref, plane_ref, cos_ref, sin_ref, factor_ref):
    own = own_ref[0]
    modes = cos_ref.shape[0]
    wide = 2 * planes
    halves = factor_ref.shape[0] // (4 * cycles * wide)
    thetas, phis, psis = (own_samples(ref, own, width) for ref in (theta_ref, phi_ref, psi_ref))
    for row in range(thetas.shape[0]):
        at = pl.ds(row * LANES, LANES)
        theta, phi, psi = (values[row : row + 1] for values in (thetas, phis, psis))
        step = min(modes, 2 * SUBLANES)

        def turn_phi(first, at=at, phi=phi, step=step):
            mode = first + lax.broadcasted_iota(jnp.int32, (step, LANES), 0)
            c, s = cos_sin((mode * phi) & (NPHI - 1), NPHI)
            cos_ref[pl.ds(first, step), at] = c
            sin_ref[pl.ds(first, step), at] = s

        if modes == step:
            turn_phi(0)
        else:
            pl.loop(0, modes, step=step)(turn_phi)
        chosen = [theta == cycle for cycle in range(cycles)]
        firsts, seconds = [], []
        for half in range(halves):
            plane = plane_ref[half * wide : (half + 1) * wide, :]
            c, s = cos_sin((plane * psi) & (NPSI - 1), NPSI)
            for pick in chosen:
                c_own, s_own = jnp.where(pick, c, 0.0), jnp.where(pick, s, 0.0)
                firsts += [c_own, -s_own]
                seconds += [s_own, c_own]
        for i, rows in enumerate((firsts, seconds)):
            full = jnp.concatenate(rows, axis=0)
            high = full.astype(jnp.bfloat16)
            low = (full - high.astype(jnp.float32)).astype(jnp.bfloat16)
            factor_ref[:, pl.ds((2 * row + i) * LANES, LANES)] = jnp.concatenate([high, low], axis=0)


def cubes(masks, sources, place_ref, table_ref, table_far_ref, beam_ref, beam_far_ref, *refs):
    *refs, out_ref = refs
    cycles, modes, planes, _ = table_ref.shape
    place = place_ref[0]
    blocks, kinds, each = refs[0].shape[0], refs[0].shape[2], refs[0].shape[3]
    rows, width = 2 * cycles * 2 * planes, max(modes, LANES)
    f32 = jnp.float32
    lane = lax.broadcasted_iota(jnp.int32, (rows, width), 1)

    def both(near_ref, far_ref, *at):
        return jnp.concatenate([near_ref[at], far_ref[at]], axis=0).astype(f32)

    beam = [[both(beam_ref, beam_far_ref, k, c) for c in range(kinds)] for k in range(2)]

    def one_mode(mode, sky, total):
        real = sum(sky[0][c] * beam[0][c] - sky[1][c] * beam[1][c] for c in range(kinds))
        imag = sum(sky[0][c] * beam[1][c] + sky[1][c] * beam[0][c] for c in range(kinds))
        spectra = [v.astype(jnp.bfloat16).astype(f32) for v in (real, imag)]
        tables = [both(table_ref, table_far_ref, g, mode) for g in range(cycles)]
        products = jnp.concatenate([s * t for t in tables for s in spectra], axis=0)
        return jnp.where(lane == mode, jnp.sum(products, axis=1, keepdims=True), total)

    def one_block(ref, sender, block, total):
        owner = sender ^ (block & 1)
        for level, mask in enumerate(masks):
            owner = owner ^ (((block >> (level + 1)) & 1) * mask)
        for inner in range(each):
            sky = [[ref[block, k, c, inner : inner + 1, :].astype(f32) for c in range(kinds)] for k in range(2)]
            total = one_mode(owner * each + inner, sky, total)
        return total

    total = refs[-1][...] if len(refs) > len(sources) else jnp.zeros((rows, width), f32)
    for ref, (even, odd) in zip(refs, sources):
        sender = place ^ jnp.where(place & 1 == 1, odd, even)
        if blocks <= SUBLANES:
            for block in range(blocks):
                total = one_block(ref, sender, block, total)
        else:
            total = lax.fori_loop(0, blocks, functools.partial(one_block, ref, sender), total)
    if out_ref.shape[0] == modes:
        for base in range(0, width, LANES):
            part = total[:, base : base + LANES]
            count = min(modes - base, LANES)
            out_ref[base : base + count, :] = jnp.concatenate([part, part], axis=0).T[:count]
    else:
        out_ref[...] = total


def sampled(near_ref, far_ref, cos_ref, sin_ref, factor_ref, out_ref):
    width = out_ref.shape[1]
    halves = [ref[half] for ref in (near_ref, far_ref) for half in range(ref.shape[0])]
    modes, doubled = halves[0].shape
    lane = lax.broadcasted_iota(jnp.int32, (modes, doubled), 1)
    whole = [jnp.where(lane < doubled // 2, *halves[i : i + 2]) for i in range(0, len(halves), 2)]
    high = [v.astype(jnp.bfloat16) for v in whole]
    low = [(v - h.astype(jnp.float32)).astype(jnp.bfloat16) for v, h in zip(whole, high)]
    left = jnp.concatenate(
        [jnp.concatenate(high + high, axis=1), jnp.concatenate(low + [jnp.zeros_like(v) for v in low], axis=1)], axis=0
    )
    done = []
    for row in range(out_ref.shape[0] * width // LANES):
        at = pl.ds(row * LANES, LANES)
        both = jnp.dot(left, factor_ref[:, pl.ds(2 * row * LANES, 2 * LANES)], preferred_element_type=jnp.float32)
        both = both[:modes] + both[modes:]
        done.append(jnp.sum(both[:, :LANES] * cos_ref[:, at] - both[:, LANES:] * sin_ref[:, at], axis=0, keepdims=True))
    result = jnp.concatenate(done, axis=0)
    rows = result.shape[0]
    for part in range(LANES // width):
        out_ref[part * rows : (part + 1) * rows, :] = result[:, part * width : (part + 1) * width]


def on_device(sky_alm, beam_blm, wigner, theta_index, phi_index, psi_index):
    f32, bf16 = jnp.float32, jnp.bfloat16
    groups, parts = lax.axis_size("det"), lax.axis_size("bm")
    place, own = lax.axis_index("det"), lax.axis_index("bm")
    cycles, modes, planes, _ = wigner.shape
    detectors = theta_index.shape[0]
    width = theta_index.shape[1] // parts
    samples = detectors * width

    def trade(values, det_mask, bm_mask=0, odd_mask=None):
        pairs = []
        for i in range(groups):
            mask = odd_mask if odd_mask is not None and i % 2 else det_mask
            pairs += [(i * parts + j, (i ^ mask) * parts + (j ^ bm_mask)) for j in range(parts)]
        return lax.ppermute(values, ("det", "bm"), pairs)

    sky_near = trade(sky_alm[None], 1)
    table_far = trade(wigner, 1, 1)
    beam_far = trade(beam_blm, 1, 1)
    table_near = trade(wigner, 1)
    plane_ids = kernel_call(
        functools.partial(plane_rows, planes),
        jax.ShapeDtypeStruct((parts * planes, LANES), jnp.int32),
        own.reshape(1),
        flops=10_000_000,
    )
    held = kernel_call(
        joined, jax.ShapeDtypeStruct((2,) + sky_alm.shape, bf16), sky_alm[None], sky_near, scalars=0
    )
    masks = [(1 << level) | 1 for level in range(3, groups.bit_length() - 1)]
    for mask in masks:
        held = jnp.concatenate([held, trade(held, mask)])
    sky_a = trade(held, 4, odd_mask=6)
    sky_b = trade(held, 3)
    sky_c = trade(sky_a, 1)

    rows = 2 * cycles * 2 * planes
    factors = jax.ShapeDtypeStruct((2 * parts // 2 * rows, 2 * samples), bf16)
    waves = jax.ShapeDtypeStruct((modes, samples), f32)
    factors_of = kernel_call(
        functools.partial(features, cycles, planes, width),
        [waves, waves, factors],
        own.reshape(1),
        theta_index,
        phi_index,
        psi_index,
        plane_ids,
    )

    def half_cube(outs, sources, *skies):
        tables = (table_near, table_far, beam_blm, beam_far)
        return kernel_call(functools.partial(cubes, masks, sources), outs, place.reshape(1), *tables, *skies)

    columns = jax.ShapeDtypeStruct((rows, max(modes, LANES)), f32)
    half = half_cube(columns, ((0, 0), (4, 6)), held, sky_a)
    half = half_cube(jax.ShapeDtypeStruct((modes, 2 * rows), f32), ((3, 3), (7, 5)), sky_b, sky_c, half)
    far = trade(half, 1, 2)[None]
    near = trade(half, 1)[None]
    bit = 4
    while bit < parts:
        far = jnp.concatenate([far, trade(jnp.concatenate([near, far]), 0, bit)])
        bit *= 2
    return kernel_call(
        sampled,
        jax.ShapeDtypeStruct((detectors, width), f32),
        near,
        far,
        *factors_of,
        scalars=0,
    )


def solution(mesh):
    placed = (
        P(None, None, "det", None),
        P(None, None, "bm", None),
        P("det", None, "bm", None),
        P("det", None),
        P("det", None),
        P("det", None),
    )
    return jax.shard_map(
        on_device, mesh=mesh, in_specs=placed, out_specs=P("det", "bm"), check_vma=False
    )
```

```python
import functools
import math

import jax
import jax.numpy as jnp
from jax import lax
from jax.experimental import pallas as pl
from jax.experimental.pallas import tpu as pltpu
from jax.sharding import PartitionSpec as P


NPHI = 16384
NPSI = 32
LANES = 128
SUBLANES = 8

SIN_TERMS = (1.0, -1 / 6, 1 / 120, -1 / 5040, 1 / 362880)
COS_TERMS = (1.0, -1 / 2, 1 / 24, -1 / 720, 1 / 40320)


def kernel_call(body, outs, *args, scalars=1, flops=0, scratch=()):
    spaces = [pltpu.SMEM] * scalars + [pltpu.VMEM] * (len(args) - scalars)
    return pl.pallas_call(
        body,
        out_shape=outs,
        in_specs=[pl.BlockSpec(memory_space=space) for space in spaces],
        out_specs=jax.tree.map(lambda _: pl.BlockSpec(memory_space=pltpu.VMEM), outs),
        scratch_shapes=list(scratch),
        cost_estimate=pl.CostEstimate(flops=flops, bytes_accessed=0, transcendentals=0),
        compiler_params=pltpu.CompilerParams(vmem_limit_bytes=16 << 20),
    )(*args)


def joined(near_ref, far_ref, out_ref):
    rows = near_ref.shape[0]
    out_ref[:rows] = near_ref[...]
    out_ref[rows:] = far_ref[...]


def cos_sin(steps, period):
    quarter = steps.astype(jnp.float32) * (4.0 / period)
    nearest = jnp.floor(quarter + 0.5)
    angle = (quarter - nearest) * (math.pi / 2)
    square = angle * angle
    sine, cosine = SIN_TERMS[-1], COS_TERMS[-1]
    for s_term, c_term in zip(SIN_TERMS[-2::-1], COS_TERMS[-2::-1]):
        sine, cosine = sine * square + s_term, cosine * square + c_term
    sine = sine * angle
    turn = nearest.astype(jnp.int32)
    swap, low = (turn & 1) == 1, (turn & 2) == 2
    c_abs, s_abs = jnp.where(swap, sine, cosine), jnp.where(swap, cosine, sine)
    return jnp.where(swap != low, -c_abs, c_abs), jnp.where(low, -s_abs, s_abs)


def own_samples(ref, own, width):
    values = pltpu.roll(ref[...], lax.rem(ref.shape[1] - own * width, ref.shape[1]), 1)[:, :LANES]
    packed = LANES // width
    rows = ref.shape[0] // packed
    lane = lax.broadcasted_iota(jnp.int32, (rows, LANES), 1)
    held = values[:rows]
    for part in range(1, packed):
        moved = pltpu.roll(values[part * rows : (part + 1) * rows], part * width, 1)
        held = jnp.where(lane // width == part, moved, held)
    return held


def plane_rows(planes, own_ref, out_ref):
    row = lax.broadcasted_iota(jnp.int32, out_ref.shape, 0)
    out_ref[...] = (own_ref[0] ^ (row // planes)) * planes + row % planes


def features(cycles, planes, width, own_ref, theta_ref, phi_ref, psi_ref, plane_ref, cos_ref, sin_ref, factor_ref):
    own = own_ref[0]
    modes = cos_ref.shape[0]
    wide = 2 * planes
    halves = factor_ref.shape[0] // (4 * cycles * wide)
    thetas, phis, psis = (own_samples(ref, own, width) for ref in (theta_ref, phi_ref, psi_ref))
    for row in range(thetas.shape[0]):
        at = pl.ds(row * LANES, LANES)
        theta, phi, psi = (values[row : row + 1] for values in (thetas, phis, psis))
        step = min(modes, 2 * SUBLANES)

        def turn_phi(first, at=at, phi=phi, step=step):
            mode = first + lax.broadcasted_iota(jnp.int32, (step, LANES), 0)
            c, s = cos_sin((mode * phi) & (NPHI - 1), NPHI)
            cos_ref[pl.ds(first, step), at] = c
            sin_ref[pl.ds(first, step), at] = s

        if modes == step:
            turn_phi(0)
        else:
            pl.loop(0, modes, step=step)(turn_phi)
        chosen = [theta == cycle for cycle in range(cycles)]
        rows = []
        for half in range(halves):
            plane = plane_ref[half * wide : (half + 1) * wide, :]
            c, s = cos_sin((plane * psi) & (NPSI - 1), NPSI)
            for pick in chosen:
                rows += [jnp.where(pick, c, 0.0), jnp.where(pick, -s, 0.0)]
        full = jnp.concatenate(rows, axis=0)
        high = full.astype(jnp.bfloat16)
        low = (full - high.astype(jnp.float32)).astype(jnp.bfloat16)
        factor_ref[:, at] = jnp.concatenate([high, low], axis=0)


def cubes(masks, sources, place_ref, table_ref, table_far_ref, beam_ref, beam_far_ref, *refs):
    *refs, out_ref = refs
    cycles, modes, planes, _ = table_ref.shape
    place = place_ref[0]
    blocks, kinds, each = refs[0].shape[0], refs[0].shape[2], refs[0].shape[3]
    rows, width = 2 * cycles * 2 * planes, max(modes, LANES)
    f32 = jnp.float32
    lane = lax.broadcasted_iota(jnp.int32, (rows, width), 1)

    def both(near_ref, far_ref, *at):
        return jnp.concatenate([near_ref[at], far_ref[at]], axis=0).astype(f32)

    beam = [[both(beam_ref, beam_far_ref, k, c) for c in range(kinds)] for k in range(2)]

    def one_mode(mode, sky, total):
        real = sum(sky[0][c] * beam[0][c] - sky[1][c] * beam[1][c] for c in range(kinds))
        imag = sum(sky[0][c] * beam[1][c] + sky[1][c] * beam[0][c] for c in range(kinds))
        spectra = [v.astype(jnp.bfloat16).astype(f32) for v in (real, imag)]
        tables = [both(table_ref, table_far_ref, g, mode) for g in range(cycles)]
        products = jnp.concatenate([s * t for t in tables for s in spectra], axis=0)
        return jnp.where(lane == mode, jnp.sum(products, axis=1, keepdims=True), total)

    def one_block(ref, sender, block, total):
        owner = sender ^ (block & 1)
        for level, mask in enumerate(masks):
            owner = owner ^ (((block >> (level + 1)) & 1) * mask)
        for inner in range(each):
            sky = [[ref[block, k, c, inner : inner + 1, :].astype(f32) for c in range(kinds)] for k in range(2)]
            total = one_mode(owner * each + inner, sky, total)
        return total

    total = refs[-1][...] if len(refs) > len(sources) else jnp.zeros((rows, width), f32)
    for ref, (even, odd) in zip(refs, sources):
        sender = place ^ jnp.where(place & 1 == 1, odd, even)
        if blocks <= SUBLANES:
            for block in range(blocks):
                total = one_block(ref, sender, block, total)
        else:
            total = lax.fori_loop(0, blocks, functools.partial(one_block, ref, sender), total)
    if out_ref.shape[0] == modes:
        for base in range(0, width, LANES):
            part = total[:, base : base + LANES]
            count = min(modes - base, LANES)
            out_ref[base : base + count, :] = jnp.concatenate([part, part], axis=0).T[:count]
    else:
        out_ref[...] = total


def sampled(planes, near_ref, far_ref, cos_ref, sin_ref, factor_ref, *out_refs):
    halves = [ref[half] for ref in (near_ref, far_ref) for half in range(ref.shape[0])]
    modes, doubled = halves[0].shape
    wide = 2 * planes
    lane = lax.broadcasted_iota(jnp.int32, (modes, doubled), 1)
    whole = [jnp.where(lane < doubled // 2, *halves[i : i + 2]) for i in range(0, len(halves), 2)]
    is_real = (lane // wide) % 2 == 0
    turned = [jnp.where(is_real, pltpu.roll(v, doubled - wide, 1), -pltpu.roll(v, wide, 1)) for v in whole]
    left = []
    for parts in (whole, turned):
        high = [v.astype(jnp.bfloat16) for v in parts]
        low = [(v - h.astype(jnp.float32)).astype(jnp.bfloat16) for v, h in zip(parts, high)]
        left += [jnp.concatenate(high + high, axis=1)]
        left += [jnp.concatenate(low + [jnp.zeros_like(v) for v in low], axis=1)]
    left = jnp.concatenate(left, axis=0)
    count = factor_ref.shape[1]
    step = math.gcd(count, 2 * LANES)
    done = []
    for start in range(0, count, step):
        at = pl.ds(start, step)
        both = jnp.dot(left, factor_ref[:, at], preferred_element_type=jnp.float32)
        real, imag = (both[i : i + modes] + both[i + modes : i + 2 * modes] for i in (0, 2 * modes))
        total = jnp.sum(real * cos_ref[:, at] - imag * sin_ref[:, at], axis=0, keepdims=True)
        done += [total[:, i : i + LANES] for i in range(0, step, LANES)]
    result = jnp.concatenate(done, axis=0)
    for part, out_ref in enumerate(out_refs):
        out_ref[...] = result[:, part * out_ref.shape[1] : (part + 1) * out_ref.shape[1]]


def on_device(sky_alm, beam_blm, wigner, theta_index, phi_index, psi_index):
    f32, bf16 = jnp.float32, jnp.bfloat16
    groups, parts = lax.axis_size("det"), lax.axis_size("bm")
    place, own = lax.axis_index("det"), lax.axis_index("bm")
    cycles, modes, planes, _ = wigner.shape
    detectors = theta_index.shape[0]
    width = theta_index.shape[1] // parts
    samples = detectors * width

    def trade(values, det_mask, bm_mask=0, odd_mask=None):
        pairs = []
        for i in range(groups):
            mask = odd_mask if odd_mask is not None and i % 2 else det_mask
            pairs += [(i * parts + j, (i ^ mask) * parts + (j ^ bm_mask)) for j in range(parts)]
        return lax.ppermute(values, ("det", "bm"), pairs)

    sky_near = trade(sky_alm[None], 1)
    table_far = trade(wigner, 1, 1)
    beam_far = trade(beam_blm, 1, 1)
    table_near = trade(wigner, 1)
    plane_ids = kernel_call(
        functools.partial(plane_rows, planes),
        jax.ShapeDtypeStruct((parts * planes, LANES), jnp.int32),
        own.reshape(1),
        flops=10_000_000,
    )
    held = kernel_call(
        joined, jax.ShapeDtypeStruct((2,) + sky_alm.shape, bf16), sky_alm[None], sky_near, scalars=0
    )
    masks = [(1 << level) | 1 for level in range(3, groups.bit_length() - 1)]
    for mask in masks:
        held = jnp.concatenate([held, trade(held, mask)])
    sky_a = trade(held, 4, odd_mask=6)
    sky_b = trade(held, 3)
    sky_c = trade(sky_a, 1)

    rows = 2 * cycles * 2 * planes
    factors = jax.ShapeDtypeStruct((2 * parts // 2 * rows, samples), bf16)
    waves = jax.ShapeDtypeStruct((modes, samples), f32)
    factors_of = kernel_call(
        functools.partial(features, cycles, planes, width),
        [waves, waves, factors],
        own.reshape(1),
        theta_index,
        phi_index,
        psi_index,
        plane_ids,
    )

    def half_cube(outs, sources, *skies):
        tables = (table_near, table_far, beam_blm, beam_far)
        return kernel_call(functools.partial(cubes, masks, sources), outs, place.reshape(1), *tables, *skies)

    columns = jax.ShapeDtypeStruct((rows, max(modes, LANES)), f32)
    half = half_cube(columns, ((0, 0), (4, 6)), held, sky_a)
    half = half_cube(jax.ShapeDtypeStruct((modes, 2 * rows), f32), ((3, 3), (7, 5)), sky_b, sky_c, half)
    far = trade(half, 1, 2)[None]
    near = trade(half, 1)[None]
    bit = 4
    while bit < parts:
        far = jnp.concatenate([far, trade(jnp.concatenate([near, far]), 0, bit)])
        bit *= 2
    result = kernel_call(
        functools.partial(sampled, planes),
        [jax.ShapeDtypeStruct((samples // LANES, width), f32)] * (LANES // width),
        near,
        far,
        *factors_of,
        scalars=0,
    )
    return jnp.concatenate(result)


def solution(mesh):
    placed = (
        P(None, None, "det", None),
        P(None, None, "bm", None),
        P("det", None, "bm", None),
        P("det", None),
        P("det", None),
        P("det", None),
    )
    return jax.shard_map(
        on_device, mesh=mesh, in_specs=placed, out_specs=P("det", "bm"), check_vma=False
    )
```

```python
import functools
import math

import jax
import jax.numpy as jnp
from jax import lax
from jax.experimental import pallas as pl
from jax.experimental.pallas import tpu as pltpu
from jax.sharding import PartitionSpec as P


NPHI = 16384
NPSI = 32
LANES = 128
SUBLANES = 8

SIN_TERMS = (1.0, -1 / 6, 1 / 120, -1 / 5040, 1 / 362880)
COS_TERMS = (1.0, -1 / 2, 1 / 24, -1 / 720, 1 / 40320)


def kernel_call(body, outs, *args, scalars=1, flops=0, scratch=()):
    spaces = [pltpu.SMEM] * scalars + [pltpu.VMEM] * (len(args) - scalars)
    return pl.pallas_call(
        body,
        out_shape=outs,
        in_specs=[pl.BlockSpec(memory_space=space) for space in spaces],
        out_specs=jax.tree.map(lambda _: pl.BlockSpec(memory_space=pltpu.VMEM), outs),
        scratch_shapes=list(scratch),
        cost_estimate=pl.CostEstimate(flops=flops, bytes_accessed=0, transcendentals=0),
        compiler_params=pltpu.CompilerParams(vmem_limit_bytes=16 << 20),
    )(*args)


def joined(near_ref, far_ref, out_ref):
    rows = near_ref.shape[0]
    out_ref[:rows] = near_ref[...]
    out_ref[rows:] = far_ref[...]


def cos_sin(steps, period):
    quarter = steps.astype(jnp.float32) * (4.0 / period)
    nearest = jnp.floor(quarter + 0.5)
    angle = (quarter - nearest) * (math.pi / 2)
    square = angle * angle
    sine, cosine = SIN_TERMS[-1], COS_TERMS[-1]
    for s_term, c_term in zip(SIN_TERMS[-2::-1], COS_TERMS[-2::-1]):
        sine, cosine = sine * square + s_term, cosine * square + c_term
    sine = sine * angle
    turn = nearest.astype(jnp.int32)
    swap, low = (turn & 1) == 1, (turn & 2) == 2
    c_abs, s_abs = jnp.where(swap, sine, cosine), jnp.where(swap, cosine, sine)
    return jnp.where(swap != low, -c_abs, c_abs), jnp.where(low, -s_abs, s_abs)


def own_samples(ref, own, width):
    values = pltpu.roll(ref[...], lax.rem(ref.shape[1] - own * width, ref.shape[1]), 1)[:, :LANES]
    packed = LANES // width
    rows = ref.shape[0] // packed
    lane = lax.broadcasted_iota(jnp.int32, (rows, LANES), 1)
    held = values[:rows]
    for part in range(1, packed):
        moved = pltpu.roll(values[part * rows : (part + 1) * rows], part * width, 1)
        held = jnp.where(lane // width == part, moved, held)
    return held


def away(source, odd):
    return (0, jnp.where(odd, 6, 4), 3, jnp.where(odd, 5, 7))[source]


def owner_of(masks, place, source, block):
    owner = place ^ away(source, place & 1 == 1) ^ (block & 1)
    for level, mask in enumerate(masks):
        owner = owner ^ (((block >> (level + 1)) & 1) * mask)
    return owner


def row_ids(masks, planes, each, own_ref, place_ref, plane_ref, mode_ref):
    row = lax.broadcasted_iota(jnp.int32, plane_ref.shape, 0)
    plane_ref[...] = (own_ref[0] ^ (row // planes)) * planes + row % planes
    row = lax.broadcasted_iota(jnp.int32, mode_ref.shape, 0)
    size = mode_ref.shape[0] // 4
    partner = place_ref[0] ^ 1
    blocks = [owner_of(masks, partner, source, row % size // each) for source in range(4)]
    owner = blocks[0]
    for source in range(1, 4):
        owner = jnp.where(row // size == source, blocks[source], owner)
    mode_ref[...] = owner * each + row % each


def features(cycles, planes, width, own_ref, theta_ref, phi_ref, psi_ref, plane_ref, mode_ref, cos_ref, sin_ref, factor_ref):
    own = own_ref[0]
    modes = cos_ref.shape[0]
    wide = 2 * planes
    halves = factor_ref.shape[0] // (4 * cycles * wide)
    thetas, phis, psis = (own_samples(ref, own, width) for ref in (theta_ref, phi_ref, psi_ref))
    for row in range(thetas.shape[0]):
        at = pl.ds(row * LANES, LANES)
        theta, phi, psi = (values[row : row + 1] for values in (thetas, phis, psis))
        step = min(modes, 2 * SUBLANES)

        def turn_phi(first, at=at, phi=phi, step=step):
            mode = mode_ref[pl.ds(first, step), :]
            c, s = cos_sin((mode * phi) & (NPHI - 1), NPHI)
            cos_ref[pl.ds(first, step), at] = c
            sin_ref[pl.ds(first, step), at] = s

        if modes == step:
            turn_phi(0)
        else:
            pl.loop(0, modes, step=step)(turn_phi)
        chosen = [theta == cycle for cycle in range(cycles)]
        rows = []
        for half in range(halves):
            plane = plane_ref[half * wide : (half + 1) * wide, :]
            c, s = cos_sin((plane * psi) & (NPSI - 1), NPSI)
            for pick in chosen:
                rows += [jnp.where(pick, c, 0.0), jnp.where(pick, -s, 0.0)]
        full = jnp.concatenate(rows, axis=0)
        high = full.astype(jnp.bfloat16)
        low = (full - high.astype(jnp.float32)).astype(jnp.bfloat16)
        factor_ref[:, at] = jnp.concatenate([high, low], axis=0)


def group_summed(columns, sky_of, beam_ref, table_of):
    kinds, wide = beam_ref.shape[1:3]
    sky = [[sky_of(k, c) for c in range(kinds)] for k in range(2)]
    lane = lax.broadcasted_iota(jnp.int32, (SUBLANES, LANES), 1) % columns
    total = jnp.zeros((SUBLANES, LANES), jnp.float32)
    for plane in range(wide):
        beam = [[beam_ref[k, c, plane : plane + 1, :] for c in range(kinds)] for k in range(2)]
        real = sum(sky[0][c] * beam[0][c] - sky[1][c] * beam[1][c] for c in range(kinds))
        imag = sum(sky[0][c] * beam[1][c] + sky[1][c] * beam[0][c] for c in range(kinds))
        for k, part in enumerate((real, imag)):
            spectra = part.astype(jnp.bfloat16).astype(jnp.float32)
            for g in range(columns // (2 * wide)):
                sums = jnp.sum(spectra * table_of(g, plane), axis=1, keepdims=True)
                total = jnp.where(lane == (2 * g + k) * wide + plane, sums, total)
    return total


def each_group(sky_refs, put):
    blocks, _, _, each, _ = sky_refs[0].shape
    pieces = SUBLANES // each

    def rows(blocks_of):
        def sky_of(k, c):
            return jnp.concatenate([ref[block, k, c].astype(jnp.float32) for ref, block in blocks_of], axis=0)

        return sky_of

    if blocks < pieces:
        spots = [(ref, block) for ref in sky_refs for block in range(blocks)]
        for group in range(len(spots) // pieces):
            put(group, rows(spots[group * pieces : (group + 1) * pieces]))
        return
    for i, ref in enumerate(sky_refs):

        @pl.loop(0, blocks // pieces)
        def _(group, i=i, ref=ref):
            put(i * (blocks // pieces) + group, rows([(ref, group * pieces + j) for j in range(pieces)]))


def first_modes(masks, place_ref, table_ref, table_far_ref, beam_ref, beam_far_ref, *refs):
    *sky_refs, total_ref, later_ref, beams_ref, laid_ref = refs
    cycles, modes, planes, _ = table_ref.shape
    blocks, each, wide = sky_refs[0].shape[0], sky_refs[0].shape[3], 2 * planes
    place = place_ref[0]

    def lay(source, block):
        for g in range(cycles):
            for inner in range(each):
                mode = owner_of(masks, place, source, block) * each + inner
                both = jnp.concatenate([table_ref[g, mode], table_far_ref[g, mode]], axis=0)
                row = (g * modes + (source * blocks + block) * each + inner) * wide
                laid_ref[pl.ds(row, wide), :] = both.astype(jnp.float32)

    for source in range(4):
        if blocks < SUBLANES:
            for block in range(blocks):
                lay(source, block)
        else:
            pl.loop(0, blocks)(functools.partial(lay, source))
    for k in range(2):
        for c in range(beam_ref.shape[1]):
            beams_ref[k, c] = jnp.concatenate([beam_ref[k, c], beam_far_ref[k, c]], axis=0).astype(jnp.float32)

    def table(group, g, plane):
        return laid_ref[pl.ds((g * modes + group * SUBLANES) * wide + plane, SUBLANES, stride=wide), :]

    def put(group, sky_of):
        for g in range(cycles):
            for plane in range(wide):
                later_ref[group, g, plane] = table(group + later_ref.shape[0], g, plane)
        rows = group_summed(cycles * 2 * wide, sky_of, beams_ref, functools.partial(table, group))
        total_ref[pl.ds(group * SUBLANES, SUBLANES), :] = rows

    each_group(sky_refs, put)


def last_modes(tables_ref, beams_ref, total_ref, *refs):
    *sky_refs, out_ref = refs
    rows = total_ref.shape[0]
    out_ref[:rows] = total_ref[...]

    def put(group, sky_of):
        columns = 2 * tables_ref.shape[1] * tables_ref.shape[2]
        total = group_summed(columns, sky_of, beams_ref, lambda g, plane: tables_ref[group, g, plane])
        out_ref[pl.ds(rows + group * SUBLANES, SUBLANES), :] = total

    each_group(sky_refs, put)


def sampled(planes, near_ref, far_ref, cos_ref, sin_ref, factor_ref, out_ref):
    width = out_ref.shape[1]
    halves = [ref[half] for ref in (near_ref, far_ref) for half in range(ref.shape[0])]
    modes, doubled = halves[0].shape
    wide = 2 * planes
    lane = lax.broadcasted_iota(jnp.int32, (modes, doubled), 1)
    whole = [jnp.where(lane < doubled // 2, *halves[i : i + 2]) for i in range(0, len(halves), 2)]
    is_real = (lane // wide) % 2 == 0
    turned = [jnp.where(is_real, pltpu.roll(v, doubled - wide, 1), -pltpu.roll(v, wide, 1)) for v in whole]
    left = []
    for parts in (whole, turned):
        high = [v.astype(jnp.bfloat16) for v in parts]
        low = [(v - h.astype(jnp.float32)).astype(jnp.bfloat16) for v, h in zip(parts, high)]
        left += [jnp.concatenate(high + high, axis=1)]
        left += [jnp.concatenate(low + [jnp.zeros_like(v) for v in low], axis=1)]
    left = jnp.concatenate(left, axis=0)
    count = out_ref.shape[0] * width
    step = math.gcd(count, 2 * LANES)
    done = []
    for start in range(0, count, step):
        at = pl.ds(start, step)
        both = jnp.dot(left, factor_ref[:, at], preferred_element_type=jnp.float32)
        real, imag = (both[i : i + modes] + both[i + modes : i + 2 * modes] for i in (0, 2 * modes))
        total = jnp.sum(real * cos_ref[:, at] - imag * sin_ref[:, at], axis=0, keepdims=True)
        done += [total[:, i : i + LANES] for i in range(0, step, LANES)]
    result = jnp.concatenate(done, axis=0)
    rows = result.shape[0]
    for part in range(LANES // width):
        out_ref[part * rows : (part + 1) * rows, :] = result[:, part * width : (part + 1) * width]


def on_device(sky_alm, beam_blm, wigner, theta_index, phi_index, psi_index):
    f32, bf16 = jnp.float32, jnp.bfloat16
    groups, parts = lax.axis_size("det"), lax.axis_size("bm")
    place, own = lax.axis_index("det"), lax.axis_index("bm")
    cycles, modes, planes, _ = wigner.shape
    detectors = theta_index.shape[0]
    width = theta_index.shape[1] // parts
    samples = detectors * width

    def trade(values, det_mask, bm_mask=0, odd_mask=None):
        pairs = []
        for i in range(groups):
            mask = odd_mask if odd_mask is not None and i % 2 else det_mask
            pairs += [(i * parts + j, (i ^ mask) * parts + (j ^ bm_mask)) for j in range(parts)]
        return lax.ppermute(values, ("det", "bm"), pairs)

    masks = [(1 << level) | 1 for level in range(3, groups.bit_length() - 1)]
    sky_near = trade(sky_alm[None], 1)
    table_far = trade(wigner, 1, 1)
    beam_far = trade(beam_blm, 1, 1)
    table_near = trade(wigner, 1)
    plane_ids, mode_ids = kernel_call(
        functools.partial(row_ids, masks, planes, sky_alm.shape[2]),
        [jax.ShapeDtypeStruct((length, LANES), jnp.int32) for length in (parts * planes, modes)],
        own.reshape(1),
        place.reshape(1),
        scalars=2,
        flops=10_000_000,
    )
    held = kernel_call(
        joined, jax.ShapeDtypeStruct((2,) + sky_alm.shape, bf16), sky_alm[None], sky_near, scalars=0
    )
    for mask in masks:
        held = jnp.concatenate([held, trade(held, mask)])
    sky_a = trade(held, 4, odd_mask=6)
    sky_b = trade(held, 3)
    sky_c = trade(sky_a, 1)

    rows = 2 * cycles * 2 * planes
    factors = jax.ShapeDtypeStruct((2 * parts // 2 * rows, samples), bf16)
    waves = jax.ShapeDtypeStruct((modes, samples), f32)
    factors_of = kernel_call(
        functools.partial(features, cycles, planes, width),
        [waves, waves, factors],
        own.reshape(1),
        theta_index,
        phi_index,
        psi_index,
        plane_ids,
        mode_ids,
    )
    first, tables, beams = kernel_call(
        functools.partial(first_modes, masks),
        [
            jax.ShapeDtypeStruct((modes // 2, 2 * rows), f32),
            jax.ShapeDtypeStruct((modes // 2 // SUBLANES, cycles, 2 * planes, SUBLANES, wigner.shape[3]), f32),
            jax.ShapeDtypeStruct(beam_blm.shape[:2] + (2 * planes,) + beam_blm.shape[3:], f32),
        ],
        place.reshape(1),
        table_near,
        table_far,
        beam_blm,
        beam_far,
        held,
        sky_a,
        scratch=[pltpu.VMEM((cycles * modes * 2 * planes, wigner.shape[3]), f32)],
    )
    half = kernel_call(
        last_modes, jax.ShapeDtypeStruct((modes, 2 * rows), f32), tables, beams, first, sky_b, sky_c, scalars=0
    )
    far = trade(half, 1, 2)[None]
    near = trade(half, 1)[None]
    bit = 4
    while bit < parts:
        far = jnp.concatenate([far, trade(jnp.concatenate([near, far]), 0, bit)])
        bit *= 2
    return kernel_call(
        functools.partial(sampled, planes),
        jax.ShapeDtypeStruct((detectors, width), f32),
        near,
        far,
        *factors_of,
        scalars=0,
    )


def solution(mesh):
    placed = (
        P(None, None, "det", None),
        P(None, None, "bm", None),
        P("det", None, "bm", None),
        P("det", None),
        P("det", None),
        P("det", None),
    )
    return jax.shard_map(
        on_device, mesh=mesh, in_specs=placed, out_specs=P("det", "bm"), check_vma=False
    )
```
